128 devices in a mesh: fsdp: 8 (over z_hi, y), tp: 16 (over x, z_lo, core).
Axes of the slice: x: 4, y: 4, z: 4 (z_hi: 2, z_lo: 2; z = z_hi * 2 + z_lo), core: 2. Of those that a mesh axis runs over, the one named last changes fastest.
Arguments:
- merged_weight: bfloat16 [8, 8192, 10240], P(None, ('fsdp', 'tp')), may hold values from -0.0625 to 0.0625
- hidden: bfloat16 [8, 1280, 8192], P('fsdp', None, 'tp'), may hold values from -6 to 6
- group_table: int32 [16], replicated, may hold values from 0 to 15, each once
Outputs:
- query: bfloat16 [8, 1280, 8192], P('fsdp', None, 'tp')
- keyvalue: bfloat16 [8, 1280, 4096], P('fsdp', None, 'tp')
The draws below stay inside these ranges and needn't reach their ends.
Inputs may be any that keep to these rules, and one draw needn't show every extreme that they name: `group_table`: every head group 0 .. 16 - 1 appears exactly once.
All inputs are finite; a program needn't handle non-finite values.
Results may differ from the reference program's by a relative error of at most 0.001.
Values may be sent and summed in bfloat16 or wider, within the bound.
No kernel may reach another device: no remote copies, remote signals or barrier semaphores. Data moves between devices by JAX's collectives and lax.ppermute only.
A program may use at most 128 MiB of HBM per device.

```python
import jax
import jax.numpy as jnp
import numpy as np

D = 8192
Q_HEADS = 64
KV_HEADS = 8
HEAD_DIM = 128
TOKS = 1280
LAYERS = 8
COLS = 10240
N_TP = 16


def steps_of(own_key, dims, cuts, least, largest):
    level, own = 1.0, jax.random.fold_in(own_key, 6)
    for axis_at, parts in cuts:
        draws = jnp.exp(jax.random.uniform(jax.random.fold_in(own, axis_at), (parts,), jnp.float32, least / len(cuts), largest / len(cuts)))
        level = level * jnp.repeat(draws, dims[axis_at] // parts).reshape([-1 if axis == axis_at else 1 for axis in range(len(dims))])
    return level


def gaussian(own_key, shape, deviation, bound, cuts=(), kind=jnp.bfloat16):
    entries = jax.random.normal(own_key, shape, jnp.float32) * deviation
    if len(cuts) > 0:
        entries = steps_of(own_key, shape, cuts, -0.22, 0.18) * entries
    return jnp.clip(entries, min=-bound, max=bound).astype(kind)


def setup_inputs(seed: int = 0) -> dict:
    key_list = jax.random.split(jax.random.key(seed), 4)
    return {
        "merged_weight": gaussian(key_list[0], (LAYERS, D, COLS), D ** -0.5, 0.0625, ((1, 128),)),
        "hidden": gaussian(key_list[1], (LAYERS, TOKS, D), 1.0, 6.0, ((0, 8), (2, 16))),
        "group_table": jax.random.permutation(key_list[2], N_TP).astype(jnp.int32),
    }


def kv_heads_table(groups):
    per_group = max(KV_HEADS // groups, 1)
    table = np.zeros((groups, per_group), np.int32)
    for group in range(groups):
        for inner in range(per_group):
            table[group, inner] = (group * per_group + inner) * KV_HEADS // (groups * per_group)
    return table


def reference(merged_weight, hidden, group_table):
    query_list = []
    kv_list = []
    split = Q_HEADS * HEAD_DIM
    heads = jnp.asarray(kv_heads_table(N_TP).reshape(-1), dtype=jnp.int32)
    for layer in range(LAYERS):
        product = jnp.dot(hidden[layer], merged_weight[layer], preferred_element_type=jnp.float32).astype(jnp.bfloat16)
        q_part = product[:, :split].reshape(TOKS, N_TP, -1)
        kv_part = product[:, split:].reshape(TOKS, 2, KV_HEADS, HEAD_DIM)
        kv_part = kv_part.transpose(0, 2, 1, 3)
        kv_part = jnp.take(kv_part, heads, axis=1).reshape(TOKS, N_TP, -1)
        query_list.append(jnp.take(q_part, group_table, axis=1).reshape(TOKS, -1))
        kv_list.append(jnp.take(kv_part, group_table, axis=1).reshape(TOKS, -1))
    return jnp.stack(query_list), jnp.stack(kv_list)
```

```python
import jax
import jax.numpy as jnp
from jax import lax
from jax.experimental import pallas as pl
from jax.experimental.pallas import tpu as pltpu
from jax.sharding import PartitionSpec as P

Q_HEADS = 64
KV_HEADS = 8
HEAD_DIM = 128


def regroup(weight, group_table):
    layers, rows, _ = weight.shape
    groups = group_table.shape[0]
    q_cols = Q_HEADS * HEAD_DIM
    q_width = q_cols // groups
    per_group = max(KV_HEADS // groups, 1)
    width = q_width + 2 * per_group * HEAD_DIM

    def body(table, src, dst, sem):
        def layer_step(layer, carry):
            for t in range(groups):
                group = table[t]
                q_at = pl.multiple_of(group * q_width, HEAD_DIM)
                pltpu.make_async_copy(
                    src.at[layer, :, pl.ds(q_at, q_width)],
                    dst.at[layer, t, :, pl.ds(0, q_width)],
                    sem,
                ).start()
                for j in range(per_group):
                    head = (group * per_group + j) * KV_HEADS // (groups * per_group)
                    for part in range(2):
                        at = pl.multiple_of(
                            q_cols + (part * KV_HEADS + head) * HEAD_DIM, HEAD_DIM
                        )
                        pltpu.make_async_copy(
                            src.at[layer, :, pl.ds(at, HEAD_DIM)],
                            dst.at[
                                layer,
                                t,
                                :,
                                pl.ds(q_width + (2 * j + part) * HEAD_DIM, HEAD_DIM),
                            ],
                            sem,
                        ).start()
            return carry

        lax.fori_loop(0, layers, layer_step, 0)
        pltpu.make_async_copy(dst, dst, sem).wait()

    return pl.pallas_call(
        body,
        out_shape=jax.ShapeDtypeStruct((layers, groups, rows, width), weight.dtype),
        in_specs=[
            pl.BlockSpec(memory_space=pltpu.SMEM),
            pl.BlockSpec(memory_space=pl.ANY),
        ],
        out_specs=pl.BlockSpec(memory_space=pl.ANY),
        scratch_shapes=[pltpu.SemaphoreType.DMA],
        name="regroup",
    )(group_table, weight)


def project(hidden, weight, q_width):
    parts, toks, feats = hidden.shape
    width = weight.shape[1]

    def body(h, w, q, kv, acc):
        k = pl.program_id(0)
        part = jnp.dot(h[0], w[...], preferred_element_type=jnp.float32)

        @pl.when(k == 0)
        def _():
            acc[...] = part

        @pl.when(k > 0)
        def _():
            acc[...] += part

        @pl.when(k == parts - 1)
        def _():
            q[...] = acc[:, :q_width].astype(q.dtype)
            kv[...] = acc[:, q_width:].astype(kv.dtype)

    return pl.pallas_call(
        body,
        grid=(parts,),
        in_specs=[
            pl.BlockSpec((1, toks, feats), lambda k: (k, 0, 0)),
            pl.BlockSpec((feats, width), lambda k: (k, 0)),
        ],
        out_specs=[
            pl.BlockSpec((toks, q_width), lambda k: (0, 0)),
            pl.BlockSpec((toks, width - q_width), lambda k: (0, 0)),
        ],
        out_shape=[
            jax.ShapeDtypeStruct((toks, q_width), hidden.dtype),
            jax.ShapeDtypeStruct((toks, width - q_width), hidden.dtype),
        ],
        scratch_shapes=[pltpu.VMEM((toks, width), jnp.float32)],
        compiler_params=pltpu.CompilerParams(vmem_limit_bytes=48 * 1024 * 1024),
        name="project",
    )(hidden, weight)


def shards(merged_weight, hidden, group_table):
    n_tp = lax.axis_size("tp")
    layers, rows, _ = merged_weight.shape
    sending = regroup(merged_weight, group_table)
    width = sending.shape[3]
    whole = lax.all_gather(hidden[0], "tp", axis=0)
    got = lax.all_to_all(
        sending.reshape(layers * n_tp, rows, width),
        ("fsdp", "tp"),
        split_axis=0,
        concat_axis=0,
        tiled=True,
    )
    q, kv = project(whole, got.reshape(-1, width), Q_HEADS * HEAD_DIM // n_tp)
    return q[None], kv[None]


def solution(mesh):
    return jax.shard_map(
        shards,
        mesh=mesh,
        in_specs=(P(None, ("fsdp", "tp"), None), P("fsdp", None, "tp"), P()),
        out_specs=(P("fsdp", None, "tp"), P("fsdp", None, "tp")),
        check_vma=False,
    )
```

```python
import jax
import jax.numpy as jnp
import numpy as np
from jax import lax
from jax.experimental import pallas as pl
from jax.experimental.pallas import tpu as pltpu
from jax.sharding import Mesh
from jax.sharding import PartitionSpec as P


Q_HEADS = 64
KV_HEADS = 8
HEAD_DIM = 128
X = 4
Q_COLS = Q_HEADS * HEAD_DIM
NEAR = (0, 0), (0, 1), (3, 0), (1, 0)
REST = (3, 1), (1, 1), (2, 0), (2, 1)
VMEM_BYTES = 40 * 1024 * 1024


def regroup(weight, group_table):
    layers, rows, cols = weight.shape
    groups = group_table.shape[0]
    q_width = Q_COLS // groups
    width = q_width + 2 * HEAD_DIM

    def body(table, src, dst):
        for t in range(groups):
            group = table[t]
            q_at = pl.multiple_of(group * q_width, HEAD_DIM)
            dst[0, t, :, :q_width] = src[0, :, pl.ds(q_at, q_width)]
            head = group * KV_HEADS // groups
            for part in range(2):
                at = pl.multiple_of(Q_COLS + (part * KV_HEADS + head) * HEAD_DIM, HEAD_DIM)
                to = q_width + part * HEAD_DIM
                dst[0, t, :, to : to + HEAD_DIM] = src[0, :, pl.ds(at, HEAD_DIM)]

    return pl.pallas_call(
        body,
        grid_spec=pltpu.PrefetchScalarGridSpec(
            num_scalar_prefetch=1,
            grid=(layers,),
            in_specs=[pl.BlockSpec((1, rows, cols), lambda i, table: (i, 0, 0))],
            out_specs=pl.BlockSpec(
                (1, groups, rows, width), lambda i, table: (i, 0, 0, 0)
            ),
        ),
        out_shape=jax.ShapeDtypeStruct((layers, groups, rows, width), weight.dtype),
        name="regroup",
    )(group_table, weight)


def spread(hidden):
    half, quarter = hidden.shape[0] // 2, hidden.shape[0] // 4
    swap = [(0, 1), (1, 0)]

    def move(axis, pairs, value):
        return lax.ppermute(value, axis, pairs)

    def up(value):
        return move("x", [(i, (i + 1) % X) for i in range(X)], value)

    def down(value):
        return move("x", [(i, (i - 1) % X) for i in range(X)], value)

    def across(value):
        return move("zl", swap, value)

    own = hidden[:half], hidden[half:]
    z = [across(own[i]) for i in range(2)]
    left = [up(own[i]) for i in range(2)]
    right = [down(own[i]) for i in range(2)]
    left_z = up(z[0]), across(left[1])
    right_z = down(z[0]), across(right[1])
    far = up(left[0]), down(right[1])
    far_z = [up(left_z[0][:quarter]), down(right_z[0][quarter:]), across(far[1])]
    return [own, z, left, right], [left_z, right_z, far, far_z]


def both(shards):
    out = []
    for pieces in shards:
        out += [pieces, []]
        for piece in pieces:
            out[-1].append(lax.ppermute(piece, "c", [(0, 1), (1, 0)]))
    return out


def project(offsets, shards, place, weight, before, q_width, last):
    table = np.zeros((2 * X * 2, len(shards)), np.int32)
    for at in range(len(table)):
        for n in range(len(shards)):
            (dx, dz), dc = offsets[n // 2], n % 2
            x, zl, c = at // 4, at // 2 % 2, at % 2
            table[at, n] = ((x + dx) % X) * 4 + (zl ^ dz) * 2 + (c ^ dc)
    order = lax.dynamic_index_in_dim(jnp.asarray(table), place, keepdims=False)
    feats = shards[0][0].shape[1]
    toks = sum(value.shape[0] for value in shards[0])
    width = weight.shape[1]
    flat = [value for pieces in shards for value in pieces]
    steps = len(shards) // 2
    most = max(
        len(shards[2 * k]) + len(shards[2 * k + 1]) + 2 for k in range(steps)
    )

    def body(order_ref, *refs):
        pieces, refs = list(refs[: len(flat)]), refs[len(flat) :]
        w, refs = refs[0], refs[1:]
        start = None
        if before is not None:
            start, refs = refs[0], refs[1:]
        if last:
            q, kv, h_buf, w_buf, sems, total = refs
        else:
            total, h_buf, w_buf, sems = refs
        k = pl.program_id(0)

        def copies(step):
            slot, out, at = step % 2, [], 0
            for n in range(2 * step):
                at += len(shards[n])
            for n in (2 * step, 2 * step + 1):
                col = (n % 2) * feats
                row = pl.multiple_of(order_ref[n] * feats, feats)
                out.append(
                    (w.at[pl.ds(row, feats)], w_buf.at[slot, pl.ds(col, feats)])
                )
                first = 0
                for value in shards[n]:
                    to = h_buf.at[slot, pl.ds(first, value.shape[0]), pl.ds(col, feats)]
                    out.append((pieces[at], to))
                    first += value.shape[0]
                    at += 1
            return [
                pltpu.make_async_copy(a, b, sems.at[slot, i])
                for i, (a, b) in enumerate(out)
            ]

        @pl.when(k == 0)
        def _():
            for copy in copies(0):
                copy.start()

        for step in range(steps):

            @pl.when(k == step)
            def _():
                if step + 1 < steps:
                    for copy in copies(step + 1):
                        copy.start()
                for copy in copies(step):
                    copy.wait()

        @pl.when(k == 0)
        def _():
            total[...] = jnp.zeros_like(total) if before is None else start[...]

        total[...] += jnp.dot(
            h_buf[k % 2], w_buf[k % 2], preferred_element_type=jnp.float32
        )

        if last:

            @pl.when(k == steps - 1)
            def _():
                q[...] = total[:, :q_width].astype(q.dtype)
                kv[...] = total[:, q_width:].astype(kv.dtype)

    def whole(k, *_):
        return (0, 0)

    in_specs = [pl.BlockSpec(memory_space=pl.ANY)] * (len(flat) + 1)
    scratch = [
        pltpu.VMEM((2, toks, 2 * feats), jnp.bfloat16),
        pltpu.VMEM((2, 2 * feats, width), jnp.bfloat16),
        pltpu.SemaphoreType.DMA((2, most)),
    ]
    args = [order, *flat, weight]
    if before is not None:
        in_specs.append(pl.BlockSpec((toks, width), whole))
        args.append(before)
    if not last:
        out_specs = pl.BlockSpec((toks, width), whole)
        out_shape = jax.ShapeDtypeStruct((toks, width), jnp.float32)
    else:
        scratch.append(pltpu.VMEM((toks, width), jnp.float32))
        out_specs = [
            pl.BlockSpec((toks, q_width), whole),
            pl.BlockSpec((toks, width - q_width), whole),
        ]
        out_shape = [
            jax.ShapeDtypeStruct((toks, q_width), jnp.bfloat16),
            jax.ShapeDtypeStruct((toks, width - q_width), jnp.bfloat16),
        ]
    return pl.pallas_call(
        body,
        grid_spec=pltpu.PrefetchScalarGridSpec(
            num_scalar_prefetch=1,
            grid=(steps,),
            in_specs=in_specs,
            out_specs=out_specs,
            scratch_shapes=scratch,
        ),
        out_shape=out_shape,
        compiler_params=pltpu.CompilerParams(vmem_limit_bytes=VMEM_BYTES),
        name="project",
    )(*args)


def step(merged_weight, hidden, group_table):
    axes = ("zh", "y", "x", "zl", "c")
    place = lax.axis_index(("x", "zl", "c"))
    layers, rows, _ = merged_weight.shape
    groups = group_table.shape[0]
    near, rest = spread(hidden[0])
    sending = regroup(merged_weight, group_table)
    width = sending.shape[3]
    near = both(near)
    got = lax.all_to_all(
        sending.reshape(layers * groups, rows, width),
        axes,
        split_axis=0,
        concat_axis=0,
        tiled=True,
    ).reshape(-1, width)
    q_width = Q_COLS // groups
    rest = both(rest)
    sums = project(NEAR, near, place, got, None, q_width, False)
    q, kv = project(REST, rest, place, got, sums, q_width, True)
    return q[None], kv[None]


def solution(mesh):
    axes = ("zh", "y", "x", "zl", "c")
    fine = Mesh(mesh.devices.reshape(2, 4, X, 2, 2), axes)
    spec = P(("zh", "y"), None, ("x", "zl", "c"))
    return jax.shard_map(
        step,
        mesh=fine,
        in_specs=(P(None, axes, None), spec, P()),
        out_specs=(spec, spec),
        check_vma=False,
    )
```

```python
import jax
import jax.numpy as jnp
import numpy as np
from jax import lax
from jax.experimental import pallas as pl
from jax.experimental.pallas import tpu as pltpu
from jax.sharding import Mesh
from jax.sharding import PartitionSpec as P


Q_HEADS = 64
KV_HEADS = 8
HEAD_DIM = 128
X = 4
Q_COLS = Q_HEADS * HEAD_DIM
NEAR = (0, 0), (0, 1), (3, 0), (1, 0)
REST = (3, 1), (1, 1), (2, 0), (2, 1)
VMEM_BYTES = 40 * 1024 * 1024


def regroup(weight, group_table):
    layers, rows, cols = weight.shape
    groups = group_table.shape[0]
    q_width = Q_COLS // groups
    width = q_width + 2 * HEAD_DIM

    def body(table, src, dst):
        for t in range(groups):
            group = table[t]
            q_at = pl.multiple_of(group * q_width, HEAD_DIM)
            dst[t, 0, :, :q_width] = src[0, :, pl.ds(q_at, q_width)]
            head = group * KV_HEADS // groups
            for part in range(2):
                at = pl.multiple_of(Q_COLS + (part * KV_HEADS + head) * HEAD_DIM, HEAD_DIM)
                to = q_width + part * HEAD_DIM
                dst[t, 0, :, to : to + HEAD_DIM] = src[0, :, pl.ds(at, HEAD_DIM)]

    return pl.pallas_call(
        body,
        grid_spec=pltpu.PrefetchScalarGridSpec(
            num_scalar_prefetch=1,
            grid=(layers,),
            in_specs=[pl.BlockSpec((1, rows, cols), lambda i, table: (i, 0, 0))],
            out_specs=pl.BlockSpec(
                (groups, 1, rows, width), lambda i, table: (0, i, 0, 0)
            ),
        ),
        out_shape=jax.ShapeDtypeStruct((groups, layers, rows, width), weight.dtype),
        name="regroup",
    )(group_table, weight)


def spread(hidden):
    half, quarter = hidden.shape[0] // 2, hidden.shape[0] // 4
    swap = [(0, 1), (1, 0)]

    def move(axis, pairs, value):
        return lax.ppermute(value, axis, pairs)

    def up(value):
        return move("x", [(i, (i + 1) % X) for i in range(X)], value)

    def down(value):
        return move("x", [(i, (i - 1) % X) for i in range(X)], value)

    def across(value):
        return move("zl", swap, value)

    own = hidden[:half], hidden[half:]
    z = [across(own[i]) for i in range(2)]
    left = [up(own[i]) for i in range(2)]
    right = [down(own[i]) for i in range(2)]
    left_z = up(z[0]), across(left[1])
    right_z = down(z[0]), across(right[1])
    far = up(left[0]), down(right[1])
    far_z = [up(left_z[0][:quarter]), down(right_z[0][quarter:]), across(far[1])]
    return [own, z, left, right], [left_z, right_z, far, far_z]


def both(shards):
    out = []
    for pieces in shards:
        out += [pieces, []]
        for piece in pieces:
            out[-1].append(lax.ppermute(piece, "c", [(0, 1), (1, 0)]))
    return out


def project(offsets, shards, place, weight, before, q_width, last):
    table = np.zeros((2 * X * 2, len(shards)), np.int32)
    for at in range(len(table)):
        for n in range(len(shards)):
            (dx, dz), dc = offsets[n // 2], n % 2
            x, zl, c = at // 4, at // 2 % 2, at % 2
            table[at, n] = ((x + dx) % X) * 4 + (zl ^ dz) * 2 + (c ^ dc)
    order = lax.dynamic_index_in_dim(jnp.asarray(table), place, keepdims=False)
    feats = shards[0][0].shape[1]
    toks = sum(value.shape[0] for value in shards[0])
    rows, width = weight.shape[2:]
    parts = feats // rows
    flat = [value for pieces in shards for value in pieces]
    steps = len(shards) // 2
    most = max(
        len(shards[2 * k]) + len(shards[2 * k + 1]) + 2 for k in range(steps)
    )

    def body(order_ref, *refs):
        pieces, refs = list(refs[: len(flat)]), refs[len(flat) :]
        w, refs = refs[0], refs[1:]
        start = None
        if before is not None:
            start, refs = refs[0], refs[1:]
        if last:
            q, kv, h_buf, w_buf, sems, total = refs
        else:
            total, h_buf, w_buf, sems = refs
        k = pl.program_id(0)

        def copies(step):
            slot, out, at = step % 2, [], 0
            for n in range(2 * step):
                at += len(shards[n])
            for n in (2 * step, 2 * step + 1):
                col = (n % 2) * feats
                device = order_ref[n]
                source = w.at[pl.ds(device % 2 * parts, parts), device // 2]
                out.append((source, w_buf.at[slot, pl.ds(n % 2 * parts, parts)]))
                first = 0
                for value in shards[n]:
                    to = h_buf.at[slot, pl.ds(first, value.shape[0]), pl.ds(col, feats)]
                    out.append((pieces[at], to))
                    first += value.shape[0]
                    at += 1
            return [
                pltpu.make_async_copy(a, b, sems.at[slot, i])
                for i, (a, b) in enumerate(out)
            ]

        @pl.when(k == 0)
        def _():
            for copy in copies(0):
                copy.start()

        for step in range(steps):

            @pl.when(k == step)
            def _():
                if step + 1 < steps:
                    for copy in copies(step + 1):
                        copy.start()
                for copy in copies(step):
                    copy.wait()

        @pl.when(k == 0)
        def _():
            total[...] = jnp.zeros_like(total) if before is None else start[...]

        total[...] += jnp.dot(
            h_buf[k % 2],
            w_buf[k % 2].reshape(2 * feats, width),
            preferred_element_type=jnp.float32,
        )

        if last:

            @pl.when(k == steps - 1)
            def _():
                q[...] = total[:, :q_width].astype(q.dtype)
                kv[...] = total[:, q_width:].astype(kv.dtype)

    def whole(k, *_):
        return (0, 0)

    in_specs = [pl.BlockSpec(memory_space=pl.ANY)] * (len(flat) + 1)
    scratch = [
        pltpu.VMEM((2, toks, 2 * feats), jnp.bfloat16),
        pltpu.VMEM((2, 2 * parts, rows, width), jnp.bfloat16),
        pltpu.SemaphoreType.DMA((2, most)),
    ]
    args = [order, *flat, weight]
    if before is not None:
        in_specs.append(pl.BlockSpec((toks, width), whole))
        args.append(before)
    if not last:
        out_specs = pl.BlockSpec((toks, width), whole)
        out_shape = jax.ShapeDtypeStruct((toks, width), jnp.float32)
    else:
        scratch.append(pltpu.VMEM((toks, width), jnp.float32))
        out_specs = [
            pl.BlockSpec((toks, q_width), whole),
            pl.BlockSpec((toks, width - q_width), whole),
        ]
        out_shape = [
            jax.ShapeDtypeStruct((toks, q_width), jnp.bfloat16),
            jax.ShapeDtypeStruct((toks, width - q_width), jnp.bfloat16),
        ]
    return pl.pallas_call(
        body,
        grid_spec=pltpu.PrefetchScalarGridSpec(
            num_scalar_prefetch=1,
            grid=(steps,),
            in_specs=in_specs,
            out_specs=out_specs,
            scratch_shapes=scratch,
        ),
        out_shape=out_shape,
        compiler_params=pltpu.CompilerParams(vmem_limit_bytes=VMEM_BYTES),
        name="project",
    )(*args)


def step(merged_weight, hidden, group_table):
    axes = ("x", "zl", "c", "zh", "y")
    place = lax.axis_index(("x", "zl", "c"))
    layers, rows, _ = merged_weight.shape
    groups = group_table.shape[0]
    near, rest = spread(hidden[0])
    sending = regroup(merged_weight, group_table)
    width = sending.shape[3]
    near = both(near)
    got = lax.all_to_all(
        sending.reshape(layers * groups, rows, width),
        axes,
        split_axis=0,
        concat_axis=0,
        tiled=True,
    ).reshape(groups, layers, rows, width)
    q_width = Q_COLS // groups
    rest = both(rest)
    q, kv = project(NEAR + REST, near + rest, place, got, None, q_width, True)
    return q[None], kv[None]


def solution(mesh):
    axes = ("zh", "y", "x", "zl", "c")
    fine = Mesh(mesh.devices.reshape(2, 4, X, 2, 2), axes)
    spec = P(("zh", "y"), None, ("x", "zl", "c"))
    return jax.shard_map(
        step,
        mesh=fine,
        in_specs=(P(None, axes, None), spec, P()),
        out_specs=(spec, spec),
        check_vma=False,
    )
```

```python
import jax
import jax.numpy as jnp
import numpy as np
from jax import lax
from jax.experimental import pallas as pl
from jax.experimental.pallas import tpu as pltpu
from jax.sharding import Mesh
from jax.sharding import PartitionSpec as P


Q_HEADS = 64
KV_HEADS = 8
HEAD_DIM = 128
X = 4
Q_COLS = Q_HEADS * HEAD_DIM
AXES = ("x", "zl", "zh", "c", "y")
SIZES = {"zh": 2, "y": 4, "x": X, "zl": 2, "c": 2}
SPLIT = 40
NEAR = (0, 0), (0, 1), (3, 0), (1, 0)
REST = (3, 1), (1, 1), (2, 0), (2, 1)
VMEM_BYTES = 40 * 1024 * 1024


def regroup(weight, group_table):
    layers, rows, cols = weight.shape
    groups = group_table.shape[0]
    q_width = Q_COLS // groups
    width = q_width + 2 * HEAD_DIM

    def body(table, src, dst):
        for t in range(groups):
            at = {"zh": 0, "y": 0, "x": t // 4, "zl": t // 2 % 2, "c": t % 2}
            at = tuple(at[name] for name in AXES)
            group = table[t]
            q_at = pl.multiple_of(group * q_width, HEAD_DIM)
            dst[(*at, slice(None), slice(0, q_width))] = src[0, :, pl.ds(q_at, q_width)]
            head = group * KV_HEADS // groups
            for part in range(2):
                kv_at = pl.multiple_of(
                    Q_COLS + (part * KV_HEADS + head) * HEAD_DIM, HEAD_DIM
                )
                to = q_width + part * HEAD_DIM
                dst[(*at, slice(None), slice(to, to + HEAD_DIM))] = src[
                    0, :, pl.ds(kv_at, HEAD_DIM)
                ]

    def place(i, table):
        at = {"zh": i // 4, "y": i % 4}
        return (*(at.get(name, 0) for name in AXES), 0, 0)

    shape = tuple(SIZES[name] for name in AXES)
    block = tuple(1 if name in ("zh", "y") else SIZES[name] for name in AXES)
    return pl.pallas_call(
        body,
        grid_spec=pltpu.PrefetchScalarGridSpec(
            num_scalar_prefetch=1,
            grid=(layers,),
            in_specs=[pl.BlockSpec((1, rows, cols), lambda i, table: (i, 0, 0))],
            out_specs=pl.BlockSpec((*block, rows, width), place),
        ),
        out_shape=jax.ShapeDtypeStruct((*shape, rows, width), weight.dtype),
        name="regroup",
    )(group_table, weight)


def spread(hidden):
    half = hidden.shape[0] * SPLIT // 80
    quarter = half // 2
    swap = [(0, 1), (1, 0)]

    def move(axis, pairs, value):
        return lax.ppermute(value, axis, pairs)

    def up(value):
        return move("x", [(i, (i + 1) % X) for i in range(X)], value)

    def down(value):
        return move("x", [(i, (i - 1) % X) for i in range(X)], value)

    def across(value):
        return move("zl", swap, value)

    own = hidden[:half], hidden[half:]
    z = [across(own[i]) for i in range(2)]
    left = [up(own[i]) for i in range(2)]
    right = [down(own[i]) for i in range(2)]
    left_z = up(z[0]), across(left[1])
    right_z = down(z[0]), across(right[1])
    far = up(left[0]), down(right[1])
    far_z = [up(left_z[0][:quarter]), down(right_z[0][quarter:]), across(far[1])]
    return [own, z, left, right], [left_z, right_z, far, far_z]


def both(shards):
    out = []
    for pieces in shards:
        out += [pieces, []]
        for piece in pieces:
            out[-1].append(lax.ppermute(piece, "c", [(0, 1), (1, 0)]))
    return out


def project(offsets, shards, place, weight, q_width):
    table = np.zeros((2 * X * 2, len(shards)), np.int32)
    for at in range(len(table)):
        for n in range(len(shards)):
            (dx, dz), dc = offsets[n // 2], n % 2
            x, zl, c = at // 4, at // 2 % 2, at % 2
            table[at, n] = ((x + dx) % X) * 4 + (zl ^ dz) * 2 + (c ^ dc)
    order = lax.dynamic_index_in_dim(jnp.asarray(table), place, keepdims=False)
    feats = shards[0][0].shape[1]
    toks = sum(value.shape[0] for value in shards[0])
    rows, width = weight.shape[5:]
    flat = [value for pieces in shards for value in pieces]
    steps = len(shards) // 2
    most = max(
        len(shards[2 * k]) + len(shards[2 * k + 1]) + 2 for k in range(steps)
    )

    def body(order_ref, *refs):
        pieces, refs = list(refs[: len(flat)]), refs[len(flat) :]
        w, refs = refs[0], refs[1:]
        q, kv, h_buf, w_buf, sems, total = refs
        k = pl.program_id(0)

        def copies(step):
            slot, out, at = step % 2, [], 0
            for n in range(2 * step):
                at += len(shards[n])
            for n in (2 * step, 2 * step + 1):
                col = (n % 2) * feats
                device = order_ref[n]
                pick = {"zh": device // 8, "y": device // 2 % 4}
                pick["x"] = pl.ds(device % 2 * 2, 2)
                source = w.at[tuple(pick.get(name, slice(None)) for name in AXES)]
                out.append((source, w_buf.at[slot, n % 2]))
                first = 0
                for value in shards[n]:
                    to = h_buf.at[slot, pl.ds(first, value.shape[0]), pl.ds(col, feats)]
                    out.append((pieces[at], to))
                    first += value.shape[0]
                    at += 1
            return [
                pltpu.make_async_copy(a, b, sems.at[slot, i])
                for i, (a, b) in enumerate(out)
            ]

        @pl.when(k == 0)
        def _():
            for copy in copies(0):
                copy.start()

        for step in range(steps):

            @pl.when(k == step)
            def _():
                if step + 1 < steps:
                    for copy in copies(step + 1):
                        copy.start()
                for copy in copies(step):
                    copy.wait()

        def product():
            return jnp.dot(
                h_buf[k % 2],
                w_buf[k % 2].reshape(2 * feats, width),
                preferred_element_type=jnp.float32,
            )

        @pl.when(k == 0)
        def _():
            total[...] = product()

        @pl.when((k > 0) & (k < steps - 1))
        def _():
            total[...] += product()

        @pl.when(k == steps - 1)
        def _():
            done = total[...] + product()
            q[...] = done[:, :q_width].astype(q.dtype)
            kv[...] = done[:, q_width:].astype(kv.dtype)

    def whole(k, *_):
        return (0, 0)

    in_specs = [pl.BlockSpec(memory_space=pl.ANY)] * (len(flat) + 1)
    scratch = [
        pltpu.VMEM((2, toks, 2 * feats), jnp.bfloat16),
        pltpu.VMEM((2, 2, 2, 2, 2, rows, width), jnp.bfloat16),
        pltpu.SemaphoreType.DMA((2, most)),
        pltpu.VMEM((toks, width), jnp.float32),
    ]
    args = [order, *flat, weight]
    out_specs = [
        pl.BlockSpec((toks, q_width), whole),
        pl.BlockSpec((toks, width - q_width), whole),
    ]
    out_shape = [
        jax.ShapeDtypeStruct((toks, q_width), jnp.bfloat16),
        jax.ShapeDtypeStruct((toks, width - q_width), jnp.bfloat16),
    ]
    return pl.pallas_call(
        body,
        grid_spec=pltpu.PrefetchScalarGridSpec(
            num_scalar_prefetch=1,
            grid=(steps,),
            in_specs=in_specs,
            out_specs=out_specs,
            scratch_shapes=scratch,
        ),
        out_shape=out_shape,
        compiler_params=pltpu.CompilerParams(vmem_limit_bytes=VMEM_BYTES),
        name="project",
    )(*args)


def step(merged_weight, hidden, group_table):
    place = lax.axis_index(("x", "zl", "c"))
    near, rest = spread(hidden[0])
    sending = regroup(merged_weight, group_table)
    near = both(near)
    got = lax.all_to_all(
        sending.reshape(-1, *sending.shape[5:]),
        AXES,
        split_axis=0,
        concat_axis=0,
        tiled=True,
    ).reshape(sending.shape)
    q_width = Q_COLS // group_table.shape[0]
    rest = both(rest)
    q, kv = project(NEAR + REST, near + rest, place, got, q_width)
    return q[None], kv[None]


def solution(mesh):
    axes = ("zh", "y", "x", "zl", "c")
    fine = Mesh(mesh.devices.reshape(2, 4, X, 2, 2), axes)
    spec = P(("zh", "y"), None, ("x", "zl", "c"))
    return jax.shard_map(
        step,
        mesh=fine,
        in_specs=(P(None, axes, None), spec, P()),
        out_specs=(spec, spec),
        check_vma=False,
    )
```

```python
import jax
import jax.numpy as jnp
import numpy as np
from jax import lax
from jax.experimental import pallas as pl
from jax.experimental.pallas import tpu as pltpu
from jax.sharding import Mesh
from jax.sharding import PartitionSpec as P


Q_HEADS = 64
KV_HEADS = 8
HEAD_DIM = 128
X = 4
Q_COLS = Q_HEADS * HEAD_DIM
AXES = ("zl", "zh", "x", "c", "y")
SIZES = {"zh": 2, "y": 4, "x": X, "zl": 2, "c": 2}
SPLIT = 42
NEAR = (0, 0), (0, 1), (3, 0), (1, 0)
REST = (3, 1), (1, 1), (2, 0), (2, 1)
VMEM_BYTES = 40 * 1024 * 1024


def regroup(weight, group_table):
    layers, rows, cols = weight.shape
    groups = group_table.shape[0]
    q_width = Q_COLS // groups
    width = q_width + 2 * HEAD_DIM

    def body(table, src, dst):
        for t in range(groups):
            at = {"zh": 0, "y": 0, "x": t // 4, "zl": t // 2 % 2, "c": t % 2}
            at = tuple(at[name] for name in AXES)
            group = table[t]
            q_at = pl.multiple_of(group * q_width, HEAD_DIM)
            dst[(*at, slice(None), slice(0, q_width))] = src[0, :, pl.ds(q_at, q_width)]
            head = group * KV_HEADS // groups
            for part in range(2):
                kv_at = pl.multiple_of(
                    Q_COLS + (part * KV_HEADS + head) * HEAD_DIM, HEAD_DIM
                )
                to = q_width + part * HEAD_DIM
                dst[(*at, slice(None), slice(to, to + HEAD_DIM))] = src[
                    0, :, pl.ds(kv_at, HEAD_DIM)
                ]

    def place(i, table):
        at = {"zh": i // 4, "y": i % 4}
        return (*(at.get(name, 0) for name in AXES), 0, 0)

    shape = tuple(SIZES[name] for name in AXES)
    block = tuple(1 if name in ("zh", "y") else SIZES[name] for name in AXES)
    return pl.pallas_call(
        body,
        grid_spec=pltpu.PrefetchScalarGridSpec(
            num_scalar_prefetch=1,
            grid=(layers,),
            in_specs=[pl.BlockSpec((1, rows, cols), lambda i, table: (i, 0, 0))],
            out_specs=pl.BlockSpec((*block, rows, width), place),
        ),
        out_shape=jax.ShapeDtypeStruct((*shape, rows, width), weight.dtype),
        name="regroup",
    )(group_table, weight)


def spread(hidden):
    half = hidden.shape[0] * SPLIT // 80
    quarter = half // 2
    swap = [(0, 1), (1, 0)]

    def move(axis, pairs, value):
        return lax.ppermute(value, axis, pairs)

    def up(value):
        return move("x", [(i, (i + 1) % X) for i in range(X)], value)

    def down(value):
        return move("x", [(i, (i - 1) % X) for i in range(X)], value)

    def across(value):
        return move("zl", swap, value)

    own = hidden[:half], hidden[half:]
    z = [across(own[i]) for i in range(2)]
    left = [up(own[i]) for i in range(2)]
    right = [down(own[i]) for i in range(2)]
    left_z = up(z[0]), across(left[1])
    right_z = down(z[0]), across(right[1])
    far = up(left[0]), down(right[1])
    far_z = [up(left_z[0][:quarter]), down(right_z[0][quarter:]), across(far[1])]
    return [own, z, left, right], [left_z, right_z, far, far_z]


def both(shards):
    out = []
    for pieces in shards:
        out += [pieces, []]
        for piece in pieces:
            out[-1].append(lax.ppermute(piece, "c", [(0, 1), (1, 0)]))
    return out


def project(offsets, shards, place, weight, q_width):
    table = np.zeros((2 * X * 2, len(shards)), np.int32)
    for at in range(len(table)):
        for n in range(len(shards)):
            (dx, dz), dc = offsets[n // 2], n % 2
            x, zl, c = at // 4, at // 2 % 2, at % 2
            table[at, n] = ((x + dx) % X) * 4 + (zl ^ dz) * 2 + (c ^ dc)
    order = lax.dynamic_index_in_dim(jnp.asarray(table), place, keepdims=False)
    feats = shards[0][0].shape[1]
    toks = sum(value.shape[0] for value in shards[0])
    rows, width = weight.shape[5:]
    flat = [value for pieces in shards for value in pieces]
    steps = len(shards) // 2
    most = max(
        len(shards[2 * k]) + len(shards[2 * k + 1]) + 4 for k in range(steps)
    )

    def body(order_ref, *refs):
        pieces, refs = list(refs[: len(flat)]), refs[len(flat) :]
        w, refs = refs[0], refs[1:]
        q, kv, h_buf, w_buf, sems, total = refs
        k = pl.program_id(0)

        def copies(step):
            slot, out, at = step % 2, [], 0
            for n in range(2 * step):
                at += len(shards[n])
            for n in (2 * step, 2 * step + 1):
                col = (n % 2) * feats
                device = order_ref[n]
                pick = {"zh": device // 8, "y": device // 2 % 4}
                pick["x"] = pl.ds(device % 2 * 2, 2)
                for zl in range(2):
                    pick["zl"] = zl
                    source = w.at[tuple(pick.get(name, slice(None)) for name in AXES)]
                    out.append((source, w_buf.at[slot, n % 2, slice(None), zl]))
                first = 0
                for value in shards[n]:
                    to = h_buf.at[slot, pl.ds(first, value.shape[0]), pl.ds(col, feats)]
                    out.append((pieces[at], to))
                    first += value.shape[0]
                    at += 1
            return [
                pltpu.make_async_copy(a, b, sems.at[slot, i])
                for i, (a, b) in enumerate(out)
            ]

        @pl.when(k == 0)
        def _():
            for copy in copies(0):
                copy.start()

        for step in range(steps):

            @pl.when(k == step)
            def _():
                if step + 1 < steps:
                    for copy in copies(step + 1):
                        copy.start()
                for copy in copies(step):
                    copy.wait()

        def product():
            return jnp.dot(
                h_buf[k % 2],
                w_buf[k % 2].reshape(2 * feats, width),
                preferred_element_type=jnp.float32,
            )

        @pl.when(k == 0)
        def _():
            total[...] = product()

        @pl.when((k > 0) & (k < steps - 1))
        def _():
            total[...] += product()

        @pl.when(k == steps - 1)
        def _():
            done = total[...] + product()
            q[...] = done[:, :q_width].astype(q.dtype)
            kv[...] = done[:, q_width:].astype(kv.dtype)

    def whole(k, *_):
        return (0, 0)

    in_specs = [pl.BlockSpec(memory_space=pl.ANY)] * (len(flat) + 1)
    scratch = [
        pltpu.VMEM((2, toks, 2 * feats), jnp.bfloat16),
        pltpu.VMEM((2, 2, 2, 2, 2, rows, width), jnp.bfloat16),
        pltpu.SemaphoreType.DMA((2, most)),
        pltpu.VMEM((toks, width), jnp.float32),
    ]
    args = [order, *flat, weight]
    out_specs = [
        pl.BlockSpec((toks, q_width), whole),
        pl.BlockSpec((toks, width - q_width), whole),
    ]
    out_shape = [
        jax.ShapeDtypeStruct((toks, q_width), jnp.bfloat16),
        jax.ShapeDtypeStruct((toks, width - q_width), jnp.bfloat16),
    ]
    return pl.pallas_call(
        body,
        grid_spec=pltpu.PrefetchScalarGridSpec(
            num_scalar_prefetch=1,
            grid=(steps,),
            in_specs=in_specs,
            out_specs=out_specs,
            scratch_shapes=scratch,
        ),
        out_shape=out_shape,
        compiler_params=pltpu.CompilerParams(vmem_limit_bytes=VMEM_BYTES),
        name="project",
    )(*args)


def step(merged_weight, hidden, group_table):
    place = lax.axis_index(("x", "zl", "c"))
    near, rest = spread(hidden[0])
    sending = regroup(merged_weight, group_table)
    near = both(near)
    got = lax.all_to_all(
        sending.reshape(-1, *sending.shape[5:]),
        AXES,
        split_axis=0,
        concat_axis=0,
        tiled=True,
    ).reshape(sending.shape)
    q_width = Q_COLS // group_table.shape[0]
    rest = both(rest)
    q, kv = project(NEAR + REST, near + rest, place, got, q_width)
    return q[None], kv[None]


def solution(mesh):
    axes = ("zh", "y", "x", "zl", "c")
    fine = Mesh(mesh.devices.reshape(2, 4, X, 2, 2), axes)
    spec = P(("zh", "y"), None, ("x", "zl", "c"))
    return jax.shard_map(
        step,
        mesh=fine,
        in_specs=(P(None, axes, None), spec, P()),
        out_specs=(spec, spec),
        check_vma=False,
    )
```

```python
import jax
import jax.numpy as jnp
import numpy as np
from jax import lax
from jax.experimental import pallas as pl
from jax.experimental.pallas import tpu as pltpu
from jax.sharding import Mesh
from jax.sharding import PartitionSpec as P


Q_HEADS = 64
KV_HEADS = 8
HEAD_DIM = 128
X = 4
Q_COLS = Q_HEADS * HEAD_DIM
AXES = ("zl", "zh", "x", "c", "y")
SIZES = {"zh": 2, "y": 4, "x": X, "zl": 2, "c": 2}
SPLIT = 42
TILES = 4
NEAR = (0, 0), (0, 1), (3, 0), (1, 0)
REST = (3, 1), (1, 1), (2, 0), (2, 1)
VMEM_BYTES = 40 * 1024 * 1024


def regroup(weight, group_table):
    layers, rows, cols = weight.shape
    groups = group_table.shape[0]
    q_width = Q_COLS // groups
    width = q_width + 2 * HEAD_DIM

    def body(table, src, dst):
        for t in range(groups):
            at = {"zh": 0, "y": 0, "x": t // 4, "zl": t // 2 % 2, "c": t % 2}
            at = tuple(at[name] for name in AXES)
            group = table[t]
            q_at = pl.multiple_of(group * q_width, HEAD_DIM)
            dst[(*at, slice(None), slice(0, q_width))] = src[0, :, pl.ds(q_at, q_width)]
            head = group * KV_HEADS // groups
            for part in range(2):
                kv_at = pl.multiple_of(
                    Q_COLS + (part * KV_HEADS + head) * HEAD_DIM, HEAD_DIM
                )
                to = q_width + part * HEAD_DIM
                dst[(*at, slice(None), slice(to, to + HEAD_DIM))] = src[
                    0, :, pl.ds(kv_at, HEAD_DIM)
                ]

    def place(i, table):
        at = {"zh": i // 4, "y": i % 4}
        return (*(at.get(name, 0) for name in AXES), 0, 0)

    shape = tuple(SIZES[name] for name in AXES)
    block = tuple(1 if name in ("zh", "y") else SIZES[name] for name in AXES)
    return pl.pallas_call(
        body,
        grid_spec=pltpu.PrefetchScalarGridSpec(
            num_scalar_prefetch=1,
            grid=(layers,),
            in_specs=[pl.BlockSpec((1, rows, cols), lambda i, table: (i, 0, 0))],
            out_specs=pl.BlockSpec((*block, rows, width), place),
        ),
        out_shape=jax.ShapeDtypeStruct((*shape, rows, width), weight.dtype),
        name="regroup",
    )(group_table, weight)


def spread(hidden):
    half = hidden.shape[0] * SPLIT // 80
    quarter = half // 2
    swap = [(0, 1), (1, 0)]

    def move(axis, pairs, value):
        return lax.ppermute(value, axis, pairs)

    def up(value):
        return move("x", [(i, (i + 1) % X) for i in range(X)], value)

    def down(value):
        return move("x", [(i, (i - 1) % X) for i in range(X)], value)

    def across(value):
        return move("zl", swap, value)

    own = hidden[:half], hidden[half:]
    z = [across(own[i]) for i in range(2)]
    left = [up(own[i]) for i in range(2)]
    right = [down(own[i]) for i in range(2)]
    left_z = up(z[0]), across(left[1])
    right_z = down(z[0]), across(right[1])
    far = up(left[0]), down(right[1])
    far_z = [up(left_z[0][:quarter]), down(right_z[0][quarter:]), across(far[1])]
    return [own, z, left, right], [left_z, right_z, far, far_z]


def both(shards):
    out = []
    for pieces in shards:
        out += [pieces, []]
        for piece in pieces:
            out[-1].append(lax.ppermute(piece, "c", [(0, 1), (1, 0)]))
    return out


def project(offsets, shards, place, weight, q_width):
    table = np.zeros((2 * X * 2, len(shards)), np.int32)
    for at in range(len(table)):
        for n in range(len(shards)):
            (dx, dz), dc = offsets[n // 2], n % 2
            x, zl, c = at // 4, at // 2 % 2, at % 2
            table[at, n] = ((x + dx) % X) * 4 + (zl ^ dz) * 2 + (c ^ dc)
    order = lax.dynamic_index_in_dim(jnp.asarray(table), place, keepdims=False)
    feats = shards[0][0].shape[1]
    toks = sum(value.shape[0] for value in shards[0])
    rows, width = weight.shape[5:]
    flat = [value for pieces in shards for value in pieces]
    steps = len(shards) // 2
    most = max(
        len(shards[2 * k]) + len(shards[2 * k + 1]) + 4 for k in range(steps)
    )

    def body(order_ref, *refs):
        pieces, refs = list(refs[: len(flat)]), refs[len(flat) :]
        w, refs = refs[0], refs[1:]
        q, kv, h_buf, w_buf, sems, total, q_out, kv_out, out_sems = refs
        k = pl.program_id(0)

        def copies(step):
            slot, out, at = step % 2, [], 0
            for n in range(2 * step):
                at += len(shards[n])
            for n in (2 * step, 2 * step + 1):
                col = (n % 2) * feats
                device = order_ref[n]
                pick = {"zh": device // 8, "y": device // 2 % 4}
                pick["x"] = pl.ds(device % 2 * 2, 2)
                for zl in range(2):
                    pick["zl"] = zl
                    source = w.at[tuple(pick.get(name, slice(None)) for name in AXES)]
                    out.append((source, w_buf.at[slot, n % 2, slice(None), zl]))
                first = 0
                for value in shards[n]:
                    to = h_buf.at[slot, pl.ds(first, value.shape[0]), pl.ds(col, feats)]
                    out.append((pieces[at], to))
                    first += value.shape[0]
                    at += 1
            return [
                pltpu.make_async_copy(a, b, sems.at[slot, i])
                for i, (a, b) in enumerate(out)
            ]

        @pl.when(k == 0)
        def _():
            for copy in copies(0):
                copy.start()

        for step in range(steps):

            @pl.when(k == step)
            def _():
                if step + 1 < steps:
                    for copy in copies(step + 1):
                        copy.start()
                for copy in copies(step):
                    copy.wait()

        def product():
            return jnp.dot(
                h_buf[k % 2],
                w_buf[k % 2].reshape(2 * feats, width),
                preferred_element_type=jnp.float32,
            )

        @pl.when(k == 0)
        def _():
            total[...] = product()

        @pl.when((k > 0) & (k < steps - 1))
        def _():
            total[...] += product()

        @pl.when(k == steps - 1)
        def _():
            outs = []
            for i in range(TILES):
                at = slice(i * toks // TILES, (i + 1) * toks // TILES)
                done = total[at] + jnp.dot(
                    h_buf[(steps - 1) % 2, at],
                    w_buf[(steps - 1) % 2].reshape(2 * feats, width),
                    preferred_element_type=jnp.float32,
                )
                q_out[at] = done[:, :q_width].astype(q.dtype)
                kv_out[at] = done[:, q_width:].astype(kv.dtype)
                outs.append(pltpu.make_async_copy(q_out.at[at], q.at[at], out_sems.at[0, i]))
                outs.append(pltpu.make_async_copy(kv_out.at[at], kv.at[at], out_sems.at[1, i]))
                outs[-2].start()
                outs[-1].start()
            for copy in outs:
                copy.wait()

    in_specs = [pl.BlockSpec(memory_space=pl.ANY)] * (len(flat) + 1)
    scratch = [
        pltpu.VMEM((2, toks, 2 * feats), jnp.bfloat16),
        pltpu.VMEM((2, 2, 2, 2, 2, rows, width), jnp.bfloat16),
        pltpu.SemaphoreType.DMA((2, most)),
        pltpu.VMEM((toks, width), jnp.float32),
        pltpu.VMEM((toks, q_width), jnp.bfloat16),
        pltpu.VMEM((toks, width - q_width), jnp.bfloat16),
        pltpu.SemaphoreType.DMA((2, TILES)),
    ]
    args = [order, *flat, weight]
    out_specs = [
        pl.BlockSpec(memory_space=pl.ANY),
        pl.BlockSpec(memory_space=pl.ANY),
    ]
    out_shape = [
        jax.ShapeDtypeStruct((toks, q_width), jnp.bfloat16),
        jax.ShapeDtypeStruct((toks, width - q_width), jnp.bfloat16),
    ]
    return pl.pallas_call(
        body,
        grid_spec=pltpu.PrefetchScalarGridSpec(
            num_scalar_prefetch=1,
            grid=(steps,),
            in_specs=in_specs,
            out_specs=out_specs,
            scratch_shapes=scratch,
        ),
        out_shape=out_shape,
        compiler_params=pltpu.CompilerParams(vmem_limit_bytes=VMEM_BYTES),
        name="project",
    )(*args)


def step(merged_weight, hidden, group_table):
    place = lax.axis_index(("x", "zl", "c"))
    near, rest = spread(hidden[0])
    sending = regroup(merged_weight, group_table)
    near = both(near)
    got = lax.all_to_all(
        sending.reshape(-1, *sending.shape[5:]),
        AXES,
        split_axis=0,
        concat_axis=0,
        tiled=True,
    ).reshape(sending.shape)
    q_width = Q_COLS // group_table.shape[0]
    rest = both(rest)
    q, kv = project(NEAR + REST, near + rest, place, got, q_width)
    return q[None], kv[None]


def solution(mesh):
    axes = ("zh", "y", "x", "zl", "c")
    fine = Mesh(mesh.devices.reshape(2, 4, X, 2, 2), axes)
    spec = P(("zh", "y"), None, ("x", "zl", "c"))
    return jax.shard_map(
        step,
        mesh=fine,
        in_specs=(P(None, axes, None), spec, P()),
        out_specs=(spec, spec),
        check_vma=False,
    )
```
